32 devices in a mesh: dp: 4 (over x, y), cp: 8 (over z, core).
Axes of the slice: x: 2, y: 2, z: 4, core: 2. Of those that a mesh axis runs over, the one named last changes fastest.
Arguments:
- q: bfloat16 [32768, 4, 128], P(('dp', 'cp')), parts along dimension 0
- k: bfloat16 [32768, 4, 128], P(('dp', 'cp')), parts along dimension 0
- v: bfloat16 [32768, 4, 128], P(('dp', 'cp')), parts along dimension 0
- o: bfloat16 [32768, 4, 128], P(('dp', 'cp')), parts along dimension 0
- do: bfloat16 [32768, 4, 128], P(('dp', 'cp')), parts along dimension 0
- lse: float32 [4, 32768], P(None, ('dp', 'cp')), parts along dimension 1
Outputs:
- output 1: bfloat16 [32768, 4, 128], P(('dp', 'cp')), parts along dimension 0
- output 2: bfloat16 [32768, 4, 128], P(('dp', 'cp')), parts along dimension 0
- output 3: bfloat16 [32768, 4, 128], P(('dp', 'cp')), parts along dimension 0
There are 4 independent parts. The reference program is written for one: setup_inputs(seed, part) draws one part's arguments, and reference() takes and returns one part's arrays. A program takes and returns all parts, laid end to end along the dimension named above; each array names one.
All inputs are finite; a program needn't handle non-finite values.
Results may differ from the reference program's by a relative error of at most 0.001.
Values are sent between devices in bfloat16 or wider.
A program may use at most 1 GiB of HBM per device.

```python
import jax
import jax.numpy as jnp
from jax import lax

TOKENS_DEV = 1024
CP = 8
H = 4
KH = 4
D = 128

T = TOKENS_DEV * CP
G = H // KH
QB = min(TOKENS_DEV, 128)
SCALE = D ** -0.5


def positions():
    r = jnp.arange(T, dtype=jnp.int32)
    return (r % TOKENS_DEV) * CP + r // TOKENS_DEV


def forward(q, k, v):
    pos = positions()
    kf = k.astype(jnp.float32)
    vf = v.astype(jnp.float32)

    def block(b):
        qb = lax.dynamic_slice_in_dim(q, b * QB, QB, 0).astype(jnp.float32).reshape(QB, KH, G, D)
        pq = lax.dynamic_slice_in_dim(pos, b * QB, QB, 0)
        s = jnp.einsum('qkgd,skd->kgqs', qb, kf) * SCALE
        s = jnp.where(pq[:, None] >= pos[None, :], s, -jnp.inf)
        m = jnp.max(s, axis=-1, keepdims=True)
        e = jnp.exp(s - m)
        l = jnp.sum(e, axis=-1, keepdims=True)
        ob = jnp.einsum('kgqs,skd->qkgd', e / l, vf).reshape(QB, H, D)
        return ob, (m + jnp.log(l))[..., 0].reshape(H, QB)

    o, lse = lax.map(block, jnp.arange(T // QB))
    return o.reshape(T, H, D).astype(jnp.bfloat16), jnp.transpose(lse, (1, 0, 2)).reshape(H, T)


def setup_inputs(seed: int = 0, part: int = 0) -> dict:
    key = jax.random.fold_in(jax.random.PRNGKey(seed), part)
    kq, kk, kv, kd = jax.random.split(key, 4)
    q = jax.random.normal(kq, (T, H, D), jnp.float32).astype(jnp.bfloat16)
    k = jax.random.normal(kk, (T, KH, D), jnp.float32).astype(jnp.bfloat16)
    v = jax.random.normal(kv, (T, KH, D), jnp.float32).astype(jnp.bfloat16)
    o, lse = forward(q, k, v)
    of = o.astype(jnp.float32)
    unit = of * lax.rsqrt(jnp.mean(of * of, axis=-1, keepdims=True) + 1e-6)
    noise = jax.random.normal(kd, (T, H, D), jnp.float32)
    do = (0.8 * unit + 0.6 * noise).astype(jnp.bfloat16)
    return {'q': q, 'k': k, 'v': v, 'o': o, 'do': do, 'lse': lse}


def reference(q, k, v, o, do, lse):
    pos = positions()
    kf = k.astype(jnp.float32)
    vf = v.astype(jnp.float32)
    delta = jnp.sum(do.astype(jnp.float32) * o.astype(jnp.float32), axis=-1)

    def step(carry, b):
        dk, dv = carry
        qb = lax.dynamic_slice_in_dim(q, b * QB, QB, 0).astype(jnp.float32).reshape(QB, KH, G, D)
        dob = lax.dynamic_slice_in_dim(do, b * QB, QB, 0).astype(jnp.float32).reshape(QB, KH, G, D)
        db = jnp.transpose(lax.dynamic_slice_in_dim(delta, b * QB, QB, 0).reshape(QB, KH, G), (1, 2, 0))[..., None]
        lb = lax.dynamic_slice_in_dim(lse, b * QB, QB, 1).reshape(KH, G, QB)[..., None]
        pq = lax.dynamic_slice_in_dim(pos, b * QB, QB, 0)
        mask = pq[:, None] >= pos[None, :]
        s = jnp.einsum('qkgd,skd->kgqs', qb, kf) * SCALE
        p = jnp.exp(jnp.where(mask, s - lb, -jnp.inf))
        pb = p.astype(jnp.bfloat16).astype(jnp.float32)
        dv = dv + jnp.einsum('kgqs,qkgd->skd', pb, dob)
        dp = jnp.einsum('qkgd,skd->kgqs', dob, vf)
        ds = (p * (dp - db)).astype(jnp.bfloat16).astype(jnp.float32)
        dqb = jnp.einsum('kgqs,skd->qkgd', ds, kf).reshape(QB, H, D) * SCALE
        dk = dk + jnp.einsum('kgqs,qkgd->skd', ds, qb)
        return (dk, dv), dqb

    zeros = jnp.zeros((T, KH, D), jnp.float32)
    (dk, dv), dq = lax.scan(step, (zeros, zeros), jnp.arange(T // QB))
    dq = dq.reshape(T, H, D).astype(jnp.bfloat16)
    return dq, (dk * SCALE).astype(jnp.bfloat16), dv.astype(jnp.bfloat16)
```

```python
import functools
import math

import jax
import jax.numpy as jnp
from jax import lax
from jax.experimental import pallas as pl
from jax.experimental.pallas import tpu as pltpu
from jax.sharding import PartitionSpec as P

F32, BF16 = jnp.float32, jnp.bfloat16
D = 128
R = 128
MESH = pl.DeviceIdType.MESH
NT = (((1,), (1,)), ((), ()))
NN = (((1,), (0,)), ((), ()))


def dot(a, b, dims=NN):
    return lax.dot_general(a, b, dims, preferred_element_type=F32)


def deinterleave(rows, heads):
    r = lax.broadcasted_iota(jnp.int32, (rows, rows), 0)
    c = lax.broadcasted_iota(jnp.int32, (rows, rows), 1)
    m = rows // heads
    return jnp.where(c == (r % m) * heads + r // m, 1.0, 0.0).astype(BF16)


def interleave(rows, heads):
    r = lax.broadcasted_iota(jnp.int32, (rows, rows), 0)
    c = lax.broadcasted_iota(jnp.int32, (rows, rows), 1)
    m = rows // heads
    return jnp.where(r == (c % m) * heads + c // m, 1.0, 0.0).astype(BF16)


def exchange_kernel(nc, q_h, do_h, k_h, v_h, o_h, lse_h, okv, oq,
                    q_r, do_r, k_r, v_r, o_r, lse_r, perm, orel,
                    sb, sbs, G, Gs, H, Hs, kt, dk_acc, dv_acc, dqo, dqp, X, skv, sq,
                    lsem, ds, dr, ss, sr, fs, fr, gs, gr, ks, kr, qs, qr, xs, xr):
    me = lax.axis_index('cp')
    z, c = me // 2, me % 2
    scale = D ** -0.5
    log2e = math.log2(math.e)
    partner = {'cp': z * 2 + (1 - c)}
    others = [lax.rem(z + i, 4) for i in (1, 2, 3)]
    home = [{'cp': zz * 2 + c} for zz in others]

    loads = [pltpu.make_async_copy(s, d, lsem.at[i]) for i, (s, d) in enumerate(
        ((q_h, q_r), (do_h, do_r), (k_h, k_r), (v_h, v_r), (o_h, o_r), (lse_h, lse_r)))]
    for x in loads:
        x.start()

    barrier = pltpu.get_barrier_semaphore()
    for dev in home + [partner]:
        pl.semaphore_signal(barrier, inc=1, device_id=dev, device_id_type=MESH)
    perm[...] = deinterleave(256, 4)
    for x in loads:
        x.wait()
    pl.semaphore_wait(barrier, 4)

    def remote(src, dst, ssem, rsem, dev):
        return pltpu.make_async_remote_copy(src_ref=src, dst_ref=dst, send_sem=ssem, recv_sem=rsem,
                                            device_id=dev, device_id_type=MESH)

    def data(a, i):
        return remote(sb.at[others[i], a], G.at[a, z], ds.at[a, others[i]], dr.at[a, z], home[i])

    def stat(a, i):
        return remote(sbs.at[others[i], a], Gs.at[a, z], ss.at[a, others[i]], sr.at[a, z], home[i])

    def data_in(a, i):
        return remote(sb.at[others[i], a], G.at[a, others[i]], ds.at[a, others[i]], dr.at[a, others[i]], home[i])

    def stat_in(a, i):
        return remote(sbs.at[others[i], a], Gs.at[a, others[i]], ss.at[a, others[i]], sr.at[a, others[i]], home[i])

    def fwd(a, zz):
        return remote(G.at[a, zz, pl.ds(0, 2)], H.at[a, zz], fs.at[a, zz], fr.at[a, zz], partner)

    def fwd_stat(a, zz):
        return remote(Gs.at[a, zz], Hs.at[a, zz], gs.at[a, zz], gr.at[a, zz], partner)

    def kv_out(a, i):
        return remote(skv.at[a, others[i]], okv.at[z, a], ks.at[a, others[i]], kr.at[a, z], home[i])

    def kv_in(a, i):
        return remote(skv.at[a, others[i]], okv.at[others[i], a], ks.at[a, others[i]], kr.at[a, others[i]], home[i])

    def kv_own(a):
        return pltpu.make_async_copy(skv.at[a, z], okv.at[z, a], ks.at[a, z])

    def q_out(a, i):
        return remote(sq.at[a, others[i]], oq.at[z, a], qs.at[a, others[i]], qr.at[a, z], home[i])

    def q_in(a, i):
        return remote(sq.at[a, others[i]], oq.at[others[i], a], qs.at[a, others[i]], qr.at[a, others[i]], home[i])

    def q_own(a):
        return pltpu.make_async_copy(sq.at[a, z], oq.at[z, a], qs.at[a, z])

    def cross(a):
        return remote(dqp.at[a], X.at[a], xs.at[a], xr.at[a], partner)

    @pl.loop(0, nc)
    def _(step):
        a = nc - 1 - step
        pm = perm[...]
        for b in range(2):
            rows = pl.ds(pl.multiple_of(a * 512 + b * 256, 256), 256)
            for t, ref in enumerate((q_r, do_r, k_r, v_r)):
                y = dot(pm, ref[rows, :]).astype(BF16)
                for h in range(4):
                    sb[h, a, t, b * 64:(b + 1) * 64, :] = y[h * 64:(h + 1) * 64]
            y = dot(pm, o_r[rows, :]).astype(BF16)
            for h in range(4):
                orel[h, b * 64:(b + 1) * 64, :] = y[h * 64:(h + 1) * 64]
        eye = (lax.broadcasted_iota(jnp.int32, (R, R), 0)
               == lax.broadcasted_iota(jnp.int32, (R, R), 1))
        for h in range(4):
            prod = dot(sb[h, a, 1], orel[h], NT)
            delta = jnp.sum(jnp.where(eye, prod, 0.0), axis=0, keepdims=True)
            sbs[h, a, 0:1, :] = lse_r[h:h + 1, pl.ds(pl.multiple_of(a * R, R), R)] * log2e
            sbs[h, a, 1:2, :] = delta
        G[a, z] = sb[z, a]
        Gs[a, z] = sbs[z, a]
        for i in range(3):
            data(a, i).start()
        for i in range(3):
            stat(a, i).start()
        fwd(a, z).start()
        fwd_stat(a, z).start()

    def tile(a, b, j, diagonal):
        src, stats, dq = (G, Gs, dqo) if j < 2 else (H, Hs, dqp)
        jj = j % 2
        kk = G[a, :, 2].reshape(4 * R, D)
        vv = G[a, :, 3].reshape(4 * R, D)
        qq = src[b, 2 * jj:2 * jj + 2, 0].reshape(2 * R, D)
        dd = src[b, 2 * jj:2 * jj + 2, 1].reshape(2 * R, D)
        row = [jnp.concatenate([stats[b, 2 * jj, r:r + 1, :], stats[b, 2 * jj + 1, r:r + 1, :]], axis=1)
               for r in range(2)]
        s = dot(kk, qq, NT) * (scale * log2e) - row[0]
        if diagonal:
            col = lax.broadcasted_iota(jnp.int32, (1, 2 * R), 1)
            tq = (col % R) * 8 + (col // R + 2 * jj) * 2 + (c if j < 2 else 1 - c)
            rw = lax.broadcasted_iota(jnp.int32, (4 * R, 1), 0)
            tk = (rw % R) * 8 + (rw // R) * 2 + c
            s = jnp.where(tq >= tk, s, -jnp.inf)
        p = jnp.exp2(s)
        dp = dot(vv, dd, NT)
        dsb = (p * (dp - row[1])).astype(BF16)
        dv_acc[...] += dot(p.astype(BF16), dd)
        dk_acc[...] += dot(dsb, qq)
        g = dot(kt[...], dsb)
        if diagonal:
            dq[b, jj] = g
        else:
            dq[b, jj] += g

    @pl.loop(0, nc)
    def _(step):
        a = nc - 1 - step
        for i in range(3):
            data_in(a, i).wait_recv()
            stat_in(a, i).wait_recv()
        for zz in others:
            fwd(a, zz).start()
            fwd_stat(a, zz).start()
        dk_acc[...] = jnp.zeros_like(dk_acc)
        dv_acc[...] = jnp.zeros_like(dv_acc)
        kt[...] = G[a, :, 2].reshape(4 * R, D).T

        @pl.loop(a + 1, nc)
        def _(b):
            for j in range(4):
                tile(a, b, j, False)

            @pl.when(a == 0)
            def _():
                cross(b).start()

        for zz in range(4):
            fwd(a, zz).wait_recv()
            fwd_stat(a, zz).wait_recv()
        for j in range(4):
            tile(a, a, j, True)
        for zz in range(4):
            skv[a, zz, 0] = (dk_acc[zz * R:(zz + 1) * R, :] * scale).astype(BF16)
            skv[a, zz, 1] = dv_acc[zz * R:(zz + 1) * R, :].astype(BF16)
        for i in range(3):
            kv_out(a, i).start()
        kv_own(a).start()

    cross(0).start()

    @pl.loop(0, nc)
    def _(step):
        b = lax.rem(step + 1, nc)
        cross(b).wait_recv()
        for jj in range(2):
            tot = ((dqo[b, jj] + X[b, jj]) * scale).astype(BF16)
            sq[b, 2 * jj] = tot[:, :R]
            sq[b, 2 * jj + 1] = tot[:, R:]
        for i in range(3):
            q_out(b, i).start()
        q_own(b).start()

    @pl.loop(0, nc)
    def _(a):
        for i in range(3):
            data(a, i).wait_send()
            stat(a, i).wait_send()
            kv_out(a, i).wait_send()
            q_out(a, i).wait_send()
            kv_in(a, i).wait_recv()
            q_in(a, i).wait_recv()
        for zz in range(4):
            fwd(a, zz).wait_send()
            fwd_stat(a, zz).wait_send()
        kv_own(a).wait()
        q_own(a).wait()
        cross(a).wait_send()


def merge_kernel(okv, oq, dq, dk, dv, p2, p5):
    @pl.when(pl.program_id(0) == 0)
    def _():
        p2[...] = interleave(256, 4)
        p5[...] = interleave(512, 4)

    for t, out in ((0, dk), (1, dv)):
        for b in range(2):
            x = jnp.concatenate([okv[h, 0, t, b * 64:(b + 1) * 64, :] for h in range(4)], axis=0)
            out[b * 256:(b + 1) * 256, :] = dot(p2[...], x).astype(BF16)
    x = jnp.concatenate([oq[h, 0] for h in range(4)], axis=1)
    dq[...] = dot(p5[...], x, NT).astype(BF16)


def solution(mesh):
    rows = P(('dp', 'cp'))
    cols = P(None, ('dp', 'cp'))

    def local(q, k, v, o, do, lse):
        n, h, d = q.shape
        nc = n // R
        flat = [x.reshape(n * h, d) for x in (q, do, k, v, o)]
        any_ = pl.BlockSpec(memory_space=pl.ANY)
        sem = pltpu.SemaphoreType.DMA
        okv, oq = pl.pallas_call(
            functools.partial(exchange_kernel, nc),
            out_shape=(jax.ShapeDtypeStruct((4, nc, 2, R, D), BF16),
                       jax.ShapeDtypeStruct((4, nc, D, R), BF16)),
            in_specs=[any_] * 6,
            out_specs=(any_, any_),
            scratch_shapes=[pltpu.VMEM((n * h, d), BF16)] * 5 + [
                pltpu.VMEM((4, n), F32),
                pltpu.VMEM((256, 256), BF16),
                pltpu.VMEM((4, R, D), BF16),
                pltpu.VMEM((4, nc, 4, R, D), BF16),
                pltpu.VMEM((4, nc, 8, R), F32),
                pltpu.VMEM((nc, 4, 4, R, D), BF16),
                pltpu.VMEM((nc, 4, 8, R), F32),
                pltpu.VMEM((nc, 4, 2, R, D), BF16),
                pltpu.VMEM((nc, 4, 8, R), F32),
                pltpu.VMEM((D, 4 * R), BF16),
                pltpu.VMEM((4 * R, D), F32),
                pltpu.VMEM((4 * R, D), F32),
                pltpu.VMEM((nc, 2, D, 2 * R), F32),
                pltpu.VMEM((nc, 2, D, 2 * R), F32),
                pltpu.VMEM((nc, 2, D, 2 * R), F32),
                pltpu.VMEM((nc, 4, 2, R, D), BF16),
                pltpu.VMEM((nc, 4, D, R), BF16),
                sem((6,)),
            ] + [sem((nc, 4))] * 12 + [sem((nc,))] * 2,
            compiler_params=pltpu.CompilerParams(collective_id=0, has_side_effects=True,
                                                 vmem_limit_bytes=56 * 2 ** 20),
            name='exchange',
        )(*flat, lse)
        dq, dk, dv = pl.pallas_call(
            merge_kernel,
            grid=(nc,),
            out_shape=(jax.ShapeDtypeStruct((n * h, d), BF16),) * 3,
            in_specs=[pl.BlockSpec((4, 1, 2, R, D), lambda a: (0, a, 0, 0, 0)),
                      pl.BlockSpec((4, 1, D, R), lambda a: (0, a, 0, 0))],
            out_specs=(pl.BlockSpec((4 * R, D), lambda a: (a, 0)),) * 3,
            scratch_shapes=[pltpu.VMEM((256, 256), BF16), pltpu.VMEM((512, 512), BF16)],
            name='merge',
        )(okv, oq)
        return tuple(x.reshape(n, h, d) for x in (dq, dk, dv))

    return jax.shard_map(local, mesh=mesh,
                         in_specs=(rows, rows, rows, rows, rows, cols),
                         out_specs=(rows, rows, rows), check_vma=False)
```

```python
import functools
import math

import jax
import jax.numpy as jnp
from jax import lax
from jax.experimental import pallas as pl
from jax.experimental.pallas import tpu as pltpu
from jax.sharding import PartitionSpec as P

F32, BF16 = jnp.float32, jnp.bfloat16
D = 128
R = 128
MESH = pl.DeviceIdType.MESH
NT = (((1,), (1,)), ((), ()))
NN = (((1,), (0,)), ((), ()))


def dot(a, b, dims=NN):
    return lax.dot_general(a, b, dims, preferred_element_type=F32)


def deinterleave(rows, heads):
    r = lax.broadcasted_iota(jnp.int32, (rows, rows), 0)
    c = lax.broadcasted_iota(jnp.int32, (rows, rows), 1)
    m = rows // heads
    return jnp.where(c == (r % m) * heads + r // m, 1.0, 0.0).astype(BF16)


def interleave(rows, heads):
    r = lax.broadcasted_iota(jnp.int32, (rows, rows), 0)
    c = lax.broadcasted_iota(jnp.int32, (rows, rows), 1)
    m = rows // heads
    return jnp.where(r == (c % m) * heads + c // m, 1.0, 0.0).astype(BF16)


def exchange_kernel(nc, q_h, do_h, k_h, v_h, o_h, lse_h, dq_o, dk_o, dv_o,
                    q_r, do_r, k_r, v_r, o_r, lse_r, perm, iperm2, iperm4, orel,
                    sb, sbs, G, Gs, H, Hs, kt, dk_acc, dv_acc, dqo, dqp, X, skv, sq, okv, oq, lse_sem, lsem, ds, dr, ss, sr, fs, fr, gs, gr, ks, kr, qs, qr, xs, xr):
    me = lax.axis_index('cp')
    z, c = me // 2, me % 2
    scale = D ** -0.5
    log2e = math.log2(math.e)
    partner = {'cp': z * 2 + (1 - c)}
    others = [lax.rem(z + i, 4) for i in (1, 2, 3)]
    home = [{'cp': zz * 2 + c} for zz in others]

    def load(a, i):
        s, d = ((q_h, q_r), (do_h, do_r), (k_h, k_r), (v_h, v_r), (o_h, o_r))[i]
        rows = pl.ds(pl.multiple_of(a * 4 * R, 4 * R), 4 * R)
        return pltpu.make_async_copy(s.at[rows], d.at[rows], lsem.at[a, i])

    lse_load = pltpu.make_async_copy(lse_h, lse_r, lse_sem.at[0])
    lse_load.start()
    barrier = pltpu.get_barrier_semaphore()
    for dev in home + [partner]:
        pl.semaphore_signal(barrier, inc=1, device_id=dev, device_id_type=MESH)

    @pl.loop(0, nc)
    def _(step):
        for i in range(5):
            load(nc - 1 - step, i).start()

    perm[...] = deinterleave(256, 4)
    iperm2[...] = interleave(256, 4)
    iperm4[...] = interleave(512, 4)
    lse_load.wait()

    def remote(src, dst, ssem, rsem, dev):
        return pltpu.make_async_remote_copy(src_ref=src, dst_ref=dst, send_sem=ssem, recv_sem=rsem,
                                            device_id=dev, device_id_type=MESH)

    def data(a, i):
        return remote(sb.at[others[i], a], G.at[a, z], ds.at[a, others[i]], dr.at[a, z], home[i])

    def stat(a, i):
        return remote(sbs.at[others[i], a], Gs.at[a, z], ss.at[a, others[i]], sr.at[a, z], home[i])

    def data_in(a, i):
        return remote(sb.at[others[i], a], G.at[a, others[i]], ds.at[a, others[i]], dr.at[a, others[i]], home[i])

    def stat_in(a, i):
        return remote(sbs.at[others[i], a], Gs.at[a, others[i]], ss.at[a, others[i]], sr.at[a, others[i]], home[i])

    def fwd(a, zz):
        return remote(G.at[a, zz, pl.ds(0, 2)], H.at[a, zz], fs.at[a, zz], fr.at[a, zz], partner)

    def fwd_stat(a, zz):
        return remote(Gs.at[a, zz], Hs.at[a, zz], gs.at[a, zz], gr.at[a, zz], partner)

    def kv_out(a, i):
        return remote(skv.at[a, others[i]], okv.at[z, a], ks.at[a, others[i]], kr.at[a, z], home[i])

    def kv_in(a, i):
        return remote(skv.at[a, others[i]], okv.at[others[i], a], ks.at[a, others[i]], kr.at[a, others[i]], home[i])

    def q_out(a, i):
        return remote(sq.at[a, others[i]], oq.at[z, a], qs.at[a, others[i]], qr.at[a, z], home[i])

    def q_in(a, i):
        return remote(sq.at[a, others[i]], oq.at[others[i], a], qs.at[a, others[i]], qr.at[a, others[i]], home[i])

    def cross(a):
        return remote(dqp.at[a], X.at[a], xs.at[a], xr.at[a], partner)

    def relayout(a):
        for i in range(5):
            load(a, i).wait()
        pm = perm[...]
        for b in range(2):
            rows = pl.ds(pl.multiple_of(a * 512 + b * 256, 256), 256)
            for t, ref in enumerate((q_r, do_r, k_r, v_r)):
                y = dot(pm, ref[rows, :]).astype(BF16)
                for h in range(4):
                    sb[h, a, t, b * 64:(b + 1) * 64, :] = y[h * 64:(h + 1) * 64]
            y = dot(pm, o_r[rows, :]).astype(BF16)
            for h in range(4):
                orel[h, b * 64:(b + 1) * 64, :] = y[h * 64:(h + 1) * 64]
        eye = (lax.broadcasted_iota(jnp.int32, (R, R), 0)
               == lax.broadcasted_iota(jnp.int32, (R, R), 1))
        for h in range(4):
            prod = dot(sb[h, a, 1], orel[h], NT)
            delta = jnp.sum(jnp.where(eye, prod, 0.0), axis=0, keepdims=True)
            sbs[h, a, 0:1, :] = lse_r[h:h + 1, pl.ds(pl.multiple_of(a * R, R), R)] * log2e
            sbs[h, a, 1:2, :] = delta
        G[a, z] = sb[z, a]
        Gs[a, z] = sbs[z, a]

    def send(a):
        for i in range(3):
            data(a, i).start()
        for i in range(3):
            stat(a, i).start()
        fwd(a, z).start()
        fwd_stat(a, z).start()

    relayout(nc - 1)
    pl.semaphore_wait(barrier, 4)
    send(nc - 1)

    @pl.loop(1, nc)
    def _(step):
        a = nc - 1 - step
        relayout(a)
        send(a)

    def tile(a, b, j, diagonal):
        src, stats, dq = (G, Gs, dqo) if j < 2 else (H, Hs, dqp)
        jj = j % 2
        kk = G[a, :, 2].reshape(4 * R, D)
        vv = G[a, :, 3].reshape(4 * R, D)
        qq = src[b, 2 * jj:2 * jj + 2, 0].reshape(2 * R, D)
        dd = src[b, 2 * jj:2 * jj + 2, 1].reshape(2 * R, D)
        row = [jnp.concatenate([stats[b, 2 * jj, r:r + 1, :], stats[b, 2 * jj + 1, r:r + 1, :]], axis=1)
               for r in range(2)]
        s = dot(kk, qq, NT) * (scale * log2e) - row[0]
        if diagonal:
            col = lax.broadcasted_iota(jnp.int32, (1, 2 * R), 1)
            tq = (col % R) * 8 + (col // R + 2 * jj) * 2 + (c if j < 2 else 1 - c)
            rw = lax.broadcasted_iota(jnp.int32, (4 * R, 1), 0)
            tk = (rw % R) * 8 + (rw // R) * 2 + c
            s = jnp.where(tq >= tk, s, -jnp.inf)
        p = jnp.exp2(s)
        dp = dot(vv, dd, NT)
        dsb = (p * (dp - row[1])).astype(BF16)
        dv_acc[...] += dot(p.astype(BF16), dd)
        dk_acc[...] += dot(dsb, qq)
        g = dot(kt[...], dsb)
        if diagonal:
            dq[b, jj] = g
        else:
            dq[b, jj] += g

    @pl.loop(0, nc)
    def _(step):
        a = nc - 1 - step
        for i in range(3):
            data_in(a, i).wait_recv()
            stat_in(a, i).wait_recv()
        for zz in others:
            fwd(a, zz).start()
            fwd_stat(a, zz).start()
        dk_acc[...] = jnp.zeros_like(dk_acc)
        dv_acc[...] = jnp.zeros_like(dv_acc)
        kt[...] = G[a, :, 2].reshape(4 * R, D).T

        @pl.loop(a + 1, nc)
        def _(b):
            for j in range(4):
                tile(a, b, j, False)

            @pl.when(a == 0)
            def _():
                cross(b).start()

        for zz in range(4):
            fwd(a, zz).wait_recv()
            fwd_stat(a, zz).wait_recv()
        for j in range(4):
            tile(a, a, j, True)
        for zz in range(4):
            skv[a, zz, 0] = (dk_acc[zz * R:(zz + 1) * R, :] * scale).astype(BF16)
            skv[a, zz, 1] = dv_acc[zz * R:(zz + 1) * R, :].astype(BF16)
        for i in range(3):
            kv_out(a, i).start()

    cross(0).start()

    @pl.loop(0, nc)
    def _(step):
        b = lax.rem(step + 1, nc)
        cross(b).wait_recv()
        for jj in range(2):
            tot = ((dqo[b, jj] + X[b, jj]) * scale).astype(BF16)
            sq[b, 2 * jj] = tot[:, :R]
            sq[b, 2 * jj + 1] = tot[:, R:]
        for i in range(3):
            q_out(b, i).start()

    @pl.loop(0, nc)
    def _(step):
        a = nc - 1 - step
        for i in range(3):
            kv_in(a, i).wait_recv()
        okv[z, a] = skv[a, z]
        for t in range(2):
            for b in range(2):
                x = jnp.concatenate([okv[h, a, t, b * 64:(b + 1) * 64, :] for h in range(4)], axis=0)
                rows = pl.ds(pl.multiple_of(a * 4 * R + b * 256, 256), 256)
                (dk_o, dv_o)[t][rows, :] = dot(iperm2[...], x).astype(BF16)

    @pl.loop(0, nc)
    def _(a):
        for i in range(3):
            data(a, i).wait_send()
            stat(a, i).wait_send()
            kv_out(a, i).wait_send()
        for zz in range(4):
            fwd(a, zz).wait_send()
            fwd_stat(a, zz).wait_send()
        cross(a).wait_send()

    @pl.loop(0, nc)
    def _(step):
        b = lax.rem(step + 1, nc)
        for i in range(3):
            q_in(b, i).wait_recv()
        oq[z, b] = sq[b, z]
        x = jnp.concatenate([oq[h, b] for h in range(4)], axis=1)
        rows = pl.ds(pl.multiple_of(b * 4 * R, 4 * R), 4 * R)
        dq_o[rows, :] = dot(iperm4[...], x, NT).astype(BF16)

    @pl.loop(0, nc)
    def _(a):
        for i in range(3):
            q_out(a, i).wait_send()


def place_kernel(*refs):
    src, dst, sems = refs[:3], refs[3:6], refs[6]
    n = src[0].shape[0] // 4
    copies = [pltpu.make_async_copy(src[t].at[pl.ds(i * n, n)], dst[t].at[pl.ds(i * n, n)], sems.at[t, i])
              for t in range(3) for i in range(4)]
    for x in copies:
        x.start()
    for x in copies:
        x.wait()


def solution(mesh):
    rows = P(('dp', 'cp'))
    cols = P(None, ('dp', 'cp'))

    def local(q, k, v, o, do, lse):
        n, h, d = q.shape
        nc = n // R
        flat = [x.reshape(n * h, d) for x in (q, do, k, v, o)]
        any_ = pl.BlockSpec(memory_space=pl.ANY)
        sem = pltpu.SemaphoreType.DMA
        vmem = pl.BlockSpec(memory_space=pltpu.VMEM)
        exchange = pl.pallas_call(
            functools.partial(exchange_kernel, nc),
            out_shape=(pltpu.VMEM((n * h, d), BF16),) * 3,
            in_specs=[any_] * 6,
            out_specs=(vmem,) * 3,
            scratch_shapes=[pltpu.VMEM((n * h, d), BF16)] * 5 + [
                pltpu.VMEM((4, n), F32),
                pltpu.VMEM((256, 256), BF16),
                pltpu.VMEM((256, 256), BF16),
                pltpu.VMEM((512, 512), BF16),
                pltpu.VMEM((4, R, D), BF16),
                pltpu.VMEM((4, nc, 4, R, D), BF16),
                pltpu.VMEM((4, nc, 2, R), F32),
                pltpu.VMEM((nc, 4, 4, R, D), BF16),
                pltpu.VMEM((nc, 4, 2, R), F32),
                pltpu.VMEM((nc, 4, 2, R, D), BF16),
                pltpu.VMEM((nc, 4, 2, R), F32),
                pltpu.VMEM((D, 4 * R), BF16),
                pltpu.VMEM((4 * R, D), F32),
                pltpu.VMEM((4 * R, D), F32),
                pltpu.VMEM((nc, 2, D, 2 * R), F32),
                pltpu.VMEM((nc, 2, D, 2 * R), F32),
                pltpu.VMEM((nc, 2, D, 2 * R), F32),
                pltpu.VMEM((nc, 4, 2, R, D), BF16),
                pltpu.VMEM((nc, 4, D, R), BF16),
                pltpu.VMEM((4, nc, 2, R, D), BF16),
                pltpu.VMEM((4, nc, D, R), BF16),
                sem((1,)), sem((nc, 5)),
            ] + [sem((nc, 4))] * 12 + [sem((nc,))] * 2,
            compiler_params=pltpu.CompilerParams(collective_id=0, has_side_effects=True,
                                                 vmem_limit_bytes=56 * 2 ** 20),
            name='exchange',
        )
        dq, dk, dv = exchange(*flat, lse)
        outs = [pltpu.with_memory_space_constraint(x, pltpu.VMEM) for x in (dq, dk, dv)]
        dq, dk, dv = pl.pallas_call(
            place_kernel,
            out_shape=(jax.ShapeDtypeStruct((n * h, d), BF16),) * 3,
            in_specs=[any_] * 3,
            out_specs=(any_,) * 3,
            scratch_shapes=[sem((3, 4))],
            name='place',
        )(*outs)
        return tuple(x.reshape(n, h, d) for x in (dq, dk, dv))

    return jax.shard_map(local, mesh=mesh,
                         in_specs=(rows, rows, rows, rows, rows, cols),
                         out_specs=(rows, rows, rows), check_vma=False)
```

```python
import functools
import math

import jax
import jax.numpy as jnp
from jax import lax
from jax.experimental import pallas as pl
from jax.experimental.pallas import tpu as pltpu
from jax.sharding import PartitionSpec as P

F32, BF16 = jnp.float32, jnp.bfloat16
D = 128
R = 128
MESH = pl.DeviceIdType.MESH
NT = (((1,), (1,)), ((), ()))
NN = (((1,), (0,)), ((), ()))


def dot(a, b, dims=NN):
    return lax.dot_general(a, b, dims, preferred_element_type=F32)


def deinterleave(rows, heads):
    r = lax.broadcasted_iota(jnp.int32, (rows, rows), 0)
    c = lax.broadcasted_iota(jnp.int32, (rows, rows), 1)
    m = rows // heads
    return jnp.where(c == (r % m) * heads + r // m, 1.0, 0.0).astype(BF16)


def interleave(rows, heads):
    r = lax.broadcasted_iota(jnp.int32, (rows, rows), 0)
    c = lax.broadcasted_iota(jnp.int32, (rows, rows), 1)
    m = rows // heads
    return jnp.where(r == (c % m) * heads + c // m, 1.0, 0.0).astype(BF16)


def exchange_kernel(nc, q_h, do_h, k_h, v_h, o_h, lse_h, dq_o, dk_o, dv_o,
                    q_r, do_r, k_r, v_r, o_r, lse_r, perm, iperm2, iperm4, orel,
                    sb, sbs, G, Gs, H, Hs, kt, dk_acc, dv_acc, dqo, dqp, X, skv, sq, okv, oq, lse_sem, lsem, ds, dr, ss, sr, fs, fr, gs, gr, ks, kr, qs, qr, xs, xr):
    me = lax.axis_index('cp')
    z, c = me // 2, me % 2
    scale = D ** -0.5
    log2e = math.log2(math.e)
    partner = {'cp': z * 2 + (1 - c)}
    near, far = z + 1 - 2 * (z % 2), 3 * (1 - z // 2)
    others = [near + c * (far - near), 6 - z - near - far, far + c * (near - far)]
    half = nc // 2
    group = (pl.ds(nc - 1, 1), pl.ds(0, nc - 1))
    home = [{'cp': zz * 2 + c} for zz in others]

    def load(a, i):
        s, d = ((q_h, q_r), (do_h, do_r), (k_h, k_r), (v_h, v_r), (o_h, o_r))[i]
        rows = pl.ds(pl.multiple_of(a * 4 * R, 4 * R), 4 * R)
        return pltpu.make_async_copy(s.at[rows], d.at[rows], lsem.at[a, i])

    lse_load = pltpu.make_async_copy(lse_h, lse_r, lse_sem.at[0])
    lse_load.start()
    barrier = pltpu.get_barrier_semaphore()
    for dev in home + [partner]:
        pl.semaphore_signal(barrier, inc=1, device_id=dev, device_id_type=MESH)

    @pl.loop(0, nc)
    def _(step):
        for i in range(5):
            load(nc - 1 - step, i).start()

    perm[...] = deinterleave(256, 4)
    lse_load.wait()

    def remote(src, dst, ssem, rsem, dev):
        return pltpu.make_async_remote_copy(src_ref=src, dst_ref=dst, send_sem=ssem, recv_sem=rsem,
                                            device_id=dev, device_id_type=MESH)

    def data(a, i):
        return remote(sb.at[others[i], a], G.at[a, z], ds.at[a, others[i]], dr.at[a, z], home[i])

    def stat(g, i):
        return remote(sbs.at[others[i], group[g]], Gs.at[z, group[g]],
                      ss.at[g, others[i]], sr.at[g, z], home[i])

    def data_in(a, i):
        return remote(sb.at[others[i], a], G.at[a, others[i]], ds.at[a, others[i]], dr.at[a, others[i]], home[i])

    def stat_in(g, i):
        return remote(sbs.at[others[i], group[g]], Gs.at[others[i], group[g]],
                      ss.at[g, others[i]], sr.at[g, others[i]], home[i])

    def fwd(a, zz):
        return remote(G.at[a, zz, pl.ds(0, 2)], H.at[a, zz], fs.at[a, zz], fr.at[a, zz], partner)

    def fwd_stat(g, zz):
        return remote(Gs.at[zz, group[g]], Hs.at[zz, group[g]], gs.at[g, zz], gr.at[g, zz], partner)

    def pair(p):
        return pl.ds(2 * p, 2)

    def kv_out(p, i):
        return remote(skv.at[others[i], pair(p)], okv.at[z, pair(p)],
                      ks.at[p, others[i]], kr.at[p, z], home[i])

    def kv_in(p, i):
        return remote(skv.at[others[i], pair(p)], okv.at[others[i], pair(p)],
                      ks.at[p, others[i]], kr.at[p, others[i]], home[i])

    def q_out(p, i):
        return remote(sq.at[others[i], pair(p)], oq.at[z, pair(p)],
                      qs.at[p, others[i]], qr.at[p, z], home[i])

    def q_in(p, i):
        return remote(sq.at[others[i], pair(p)], oq.at[others[i], pair(p)],
                      qs.at[p, others[i]], qr.at[p, others[i]], home[i])

    def cross(a):
        return remote(dqp.at[a], X.at[a], xs.at[a], xr.at[a], partner)

    def relayout(a):
        for i in range(5):
            load(a, i).wait()
        pm = perm[...]
        for b in range(2):
            rows = pl.ds(pl.multiple_of(a * 512 + b * 256, 256), 256)
            for t, ref in enumerate((q_r, do_r, k_r, v_r)):
                y = dot(pm, ref[rows, :]).astype(BF16)
                for h in range(4):
                    sb[h, a, t, b * 64:(b + 1) * 64, :] = y[h * 64:(h + 1) * 64]
            y = dot(pm, o_r[rows, :]).astype(BF16)
            for h in range(4):
                orel[h, b * 64:(b + 1) * 64, :] = y[h * 64:(h + 1) * 64]
        eye = (lax.broadcasted_iota(jnp.int32, (R, R), 0)
               == lax.broadcasted_iota(jnp.int32, (R, R), 1))
        for h in range(4):
            prod = dot(sb[h, a, 1], orel[h], NT)
            delta = jnp.sum(jnp.where(eye, prod, 0.0), axis=0, keepdims=True)
            sbs[h, a, 0:1, :] = lse_r[h:h + 1, pl.ds(pl.multiple_of(a * R, R), R)] * log2e
            sbs[h, a, 1:2, :] = delta
        G[a, z] = sb[z, a]
        Gs[z, a] = sbs[z, a]

    def send(a):
        for i in range(3):
            data(a, i).start()
        fwd(a, z).start()

    def send_stats(g):
        for i in range(3):
            stat(g, i).start()
        fwd_stat(g, z).start()

    relayout(nc - 1)
    pl.semaphore_wait(barrier, 4)
    send(nc - 1)
    send_stats(0)

    @pl.loop(1, nc)
    def _(step):
        relayout(nc - 1 - step)

    send_stats(1)

    @pl.loop(1, nc)
    def _(step):
        send(nc - 1 - step)

    iperm2[...] = interleave(256, 4)
    iperm4[...] = interleave(512, 4)

    def tile(a, b, j, diagonal):
        src, stats, dq = (G, Gs, dqo) if j < 2 else (H, Hs, dqp)
        jj = j % 2
        kk = G[a, :, 2].reshape(4 * R, D)
        vv = G[a, :, 3].reshape(4 * R, D)
        qq = src[b, 2 * jj:2 * jj + 2, 0].reshape(2 * R, D)
        dd = src[b, 2 * jj:2 * jj + 2, 1].reshape(2 * R, D)
        row = [jnp.concatenate([stats[2 * jj, b, r:r + 1, :], stats[2 * jj + 1, b, r:r + 1, :]], axis=1)
               for r in range(2)]
        s = dot(kk, qq, NT) * (scale * log2e) - row[0]
        if diagonal:
            col = lax.broadcasted_iota(jnp.int32, (1, 2 * R), 1)
            tq = (col % R) * 8 + (col // R + 2 * jj) * 2 + (c if j < 2 else 1 - c)
            rw = lax.broadcasted_iota(jnp.int32, (4 * R, 1), 0)
            tk = (rw % R) * 8 + (rw // R) * 2 + c
            s = jnp.where(tq >= tk, s, -jnp.inf)
        p = jnp.exp2(s)
        dp = dot(vv, dd, NT)
        dsb = (p * (dp - row[1])).astype(BF16)
        dv_acc[...] += dot(p.astype(BF16), dd)
        dk_acc[...] += dot(dsb, qq)
        g = dot(kt[...], dsb)
        if diagonal:
            dq[b, jj] = g
        else:
            dq[b, jj] += g

    @pl.loop(0, nc)
    def _(step):
        a = nc - 1 - step
        for i in range(3):
            data_in(a, i).wait_recv()
        for zz in others:
            fwd(a, zz).start()
        for g in range(2):
            @pl.when(step == g)
            def _():
                for i in range(3):
                    stat_in(g, i).wait_recv()
                for zz in others:
                    fwd_stat(g, zz).start()
        dk_acc[...] = jnp.zeros_like(dk_acc)
        dv_acc[...] = jnp.zeros_like(dv_acc)
        kt[...] = G[a, :, 2].reshape(4 * R, D).T

        @pl.loop(a + 1, nc)
        def _(b):
            for j in range(4):
                tile(a, b, j, False)

            @pl.when(a == 0)
            def _():
                cross(b).start()

        for zz in range(4):
            fwd(a, zz).wait_recv()
        for g in range(2):
            @pl.when(step == g)
            def _():
                for zz in range(4):
                    fwd_stat(g, zz).wait_recv()
        for j in range(4):
            tile(a, a, j, True)
        for zz in range(4):
            skv[zz, a, 0] = (dk_acc[zz * R:(zz + 1) * R, :] * scale).astype(BF16)
            skv[zz, a, 1] = dv_acc[zz * R:(zz + 1) * R, :].astype(BF16)

        @pl.when(a % 2 == 0)
        def _():
            for i in range(3):
                kv_out(a // 2, i).start()

    cross(0).start()

    @pl.loop(0, half)
    def _(step):
        p = lax.rem(step + 1, half)
        for e in range(2):
            b = 2 * p + e
            cross(b).wait_recv()
            for jj in range(2):
                tot = ((dqo[b, jj] + X[b, jj]) * scale).astype(BF16)
                sq[2 * jj, b] = tot[:, :R]
                sq[2 * jj + 1, b] = tot[:, R:]
        for i in range(3):
            q_out(p, i).start()

    @pl.loop(0, half)
    def _(step):
        p = half - 1 - step
        for i in range(3):
            kv_in(p, i).wait_recv()
        for e in range(2):
            a = 2 * p + e
            okv[z, a] = skv[z, a]
            for t in range(2):
                for b in range(2):
                    x = jnp.concatenate([okv[h, a, t, b * 64:(b + 1) * 64, :] for h in range(4)], axis=0)
                    rows = pl.ds(pl.multiple_of(a * 4 * R + b * 256, 256), 256)
                    (dk_o, dv_o)[t][rows, :] = dot(iperm2[...], x).astype(BF16)

    @pl.loop(0, nc)
    def _(a):
        for i in range(3):
            data(a, i).wait_send()
        for zz in range(4):
            fwd(a, zz).wait_send()
        cross(a).wait_send()

    for g in range(2):
        for i in range(3):
            stat(g, i).wait_send()
        for zz in range(4):
            fwd_stat(g, zz).wait_send()

    @pl.loop(0, half)
    def _(step):
        p = lax.rem(step + 1, half)
        for i in range(3):
            kv_out(p, i).wait_send()
            q_in(p, i).wait_recv()
        for e in range(2):
            b = 2 * p + e
            oq[z, b] = sq[z, b]
            x = jnp.concatenate([oq[h, b] for h in range(4)], axis=1)
            rows = pl.ds(pl.multiple_of(b * 4 * R, 4 * R), 4 * R)
            dq_o[rows, :] = dot(iperm4[...], x, NT).astype(BF16)

    @pl.loop(0, half)
    def _(p):
        for i in range(3):
            q_out(p, i).wait_send()


def place_kernel(*refs):
    src, dst, sems = refs[:3], refs[3:6], refs[6]
    n = src[0].shape[0] // 4
    copies = [pltpu.make_async_copy(src[t].at[pl.ds(i * n, n)], dst[t].at[pl.ds(i * n, n)], sems.at[t, i])
              for t in range(3) for i in range(4)]
    for x in copies:
        x.start()
    for x in copies:
        x.wait()


def solution(mesh):
    rows = P(('dp', 'cp'))
    cols = P(None, ('dp', 'cp'))

    def local(q, k, v, o, do, lse):
        n, h, d = q.shape
        nc = n // R
        flat = [x.reshape(n * h, d) for x in (q, do, k, v, o)]
        any_ = pl.BlockSpec(memory_space=pl.ANY)
        sem = pltpu.SemaphoreType.DMA
        vmem = pl.BlockSpec(memory_space=pltpu.VMEM)
        exchange = pl.pallas_call(
            functools.partial(exchange_kernel, nc),
            out_shape=(pltpu.VMEM((n * h, d), BF16),) * 3,
            in_specs=[any_] * 6,
            out_specs=(vmem,) * 3,
            scratch_shapes=[pltpu.VMEM((n * h, d), BF16)] * 5 + [
                pltpu.VMEM((4, n), F32),
                pltpu.VMEM((256, 256), BF16),
                pltpu.VMEM((256, 256), BF16),
                pltpu.VMEM((512, 512), BF16),
                pltpu.VMEM((4, R, D), BF16),
                pltpu.VMEM((4, nc, 4, R, D), BF16),
                pltpu.VMEM((4, nc, 2, R), F32),
                pltpu.VMEM((nc, 4, 4, R, D), BF16),
                pltpu.VMEM((4, nc, 2, R), F32),
                pltpu.VMEM((nc, 4, 2, R, D), BF16),
                pltpu.VMEM((4, nc, 2, R), F32),
                pltpu.VMEM((D, 4 * R), BF16),
                pltpu.VMEM((4 * R, D), F32),
                pltpu.VMEM((4 * R, D), F32),
                pltpu.VMEM((nc, 2, D, 2 * R), F32),
                pltpu.VMEM((nc, 2, D, 2 * R), F32),
                pltpu.VMEM((nc, 2, D, 2 * R), F32),
                pltpu.VMEM((4, nc, 2, R, D), BF16),
                pltpu.VMEM((4, nc, D, R), BF16),
                pltpu.VMEM((4, nc, 2, R, D), BF16),
                pltpu.VMEM((4, nc, D, R), BF16),
                sem((1,)), sem((nc, 5)),
            ] + [sem((nc, 4))] * 2 + [sem((2, 4))] * 2 + [sem((nc, 4))] * 2 + [sem((2, 4))] * 2 + [
                sem((nc // 2, 4))] * 4 + [sem((nc,))] * 2,
            compiler_params=pltpu.CompilerParams(collective_id=0, has_side_effects=True,
                                                 vmem_limit_bytes=56 * 2 ** 20),
            name='exchange',
        )
        dq, dk, dv = exchange(*flat, lse)
        outs = [pltpu.with_memory_space_constraint(x, pltpu.VMEM) for x in (dq, dk, dv)]
        dq, dk, dv = pl.pallas_call(
            place_kernel,
            out_shape=(jax.ShapeDtypeStruct((n * h, d), BF16),) * 3,
            in_specs=[any_] * 3,
            out_specs=(any_,) * 3,
            scratch_shapes=[sem((3, 4))],
            name='place',
        )(*outs)
        return tuple(x.reshape(n, h, d) for x in (dq, dk, dv))

    return jax.shard_map(local, mesh=mesh,
                         in_specs=(rows, rows, rows, rows, rows, cols),
                         out_specs=(rows, rows, rows), check_vma=False)
```

```python
import functools
import math

import jax
import jax.numpy as jnp
from jax import lax
from jax.experimental import pallas as pl
from jax.experimental.pallas import tpu as pltpu
from jax.sharding import PartitionSpec as P

F32, BF16 = jnp.float32, jnp.bfloat16
D = 128
R = 128
MESH = pl.DeviceIdType.MESH
NT = (((1,), (1,)), ((), ()))
NN = (((1,), (0,)), ((), ()))


def dot(a, b, dims=NN):
    return lax.dot_general(a, b, dims, preferred_element_type=F32)


def deinterleave(rows, heads):
    r = lax.broadcasted_iota(jnp.int32, (rows, rows), 0)
    c = lax.broadcasted_iota(jnp.int32, (rows, rows), 1)
    m = rows // heads
    return jnp.where(c == (r % m) * heads + r // m, 1.0, 0.0).astype(BF16)


def interleave(rows, heads):
    r = lax.broadcasted_iota(jnp.int32, (rows, rows), 0)
    c = lax.broadcasted_iota(jnp.int32, (rows, rows), 1)
    m = rows // heads
    return jnp.where(r == (c % m) * heads + c // m, 1.0, 0.0).astype(BF16)


def exchange_kernel(nc, q_h, do_h, k_h, v_h, o_h, lse_h, dq_o, dk_o, dv_o,
                    q_r, do_r, k_r, v_r, o_r, lse_r, perm, iperm2, iperm4, orel,
                    sb, sbs, G, Gs, H, Hs, kt, dk_acc, dv_acc, dqo, dqp, X, skv, sq, okv, oq, lse_sem, lsem, ds, dr, ss, sr, fs, fr, gs, gr, ks, kr, qs, qr, xs, xr):
    me = lax.axis_index('cp')
    z, c = me // 2, me % 2
    scale = D ** -0.5
    log2e = math.log2(math.e)
    partner = {'cp': z * 2 + (1 - c)}
    near, far = z + 1 - 2 * (z % 2), 3 * (1 - z // 2)
    others = [near + c * (far - near), 6 - z - near - far, far + c * (near - far)]
    half = nc // 2
    group = (pl.ds(nc - 1, 1), pl.ds(0, nc - 1))
    home = [{'cp': zz * 2 + c} for zz in others]
    q_to = [far, 6 - z - near - far, near]
    q_home = [{'cp': zz * 2 + c} for zz in q_to]

    def load(a, i):
        s, d = ((q_h, q_r), (do_h, do_r), (k_h, k_r), (v_h, v_r), (o_h, o_r))[i]
        rows = pl.ds(pl.multiple_of(a * 4 * R, 4 * R), 4 * R)
        return pltpu.make_async_copy(s.at[rows], d.at[rows], lsem.at[a, i])

    lse_load = pltpu.make_async_copy(lse_h, lse_r, lse_sem.at[0])
    lse_load.start()
    barrier = pltpu.get_barrier_semaphore()
    for dev in home + [partner]:
        pl.semaphore_signal(barrier, inc=1, device_id=dev, device_id_type=MESH)

    @pl.loop(0, nc)
    def _(step):
        for i in range(5):
            load(nc - 1 - step, i).start()

    perm[...] = deinterleave(256, 4)
    lse_load.wait()

    def remote(src, dst, ssem, rsem, dev):
        return pltpu.make_async_remote_copy(src_ref=src, dst_ref=dst, send_sem=ssem, recv_sem=rsem,
                                            device_id=dev, device_id_type=MESH)

    def data(a, i):
        return remote(sb.at[others[i], a], G.at[a, z], ds.at[a, others[i]], dr.at[a, z], home[i])

    def stat(g, i):
        return remote(sbs.at[others[i], group[g]], Gs.at[z, group[g]],
                      ss.at[g, others[i]], sr.at[g, z], home[i])

    def data_in(a, i):
        return remote(sb.at[others[i], a], G.at[a, others[i]], ds.at[a, others[i]], dr.at[a, others[i]], home[i])

    def stat_in(g, i):
        return remote(sbs.at[others[i], group[g]], Gs.at[others[i], group[g]],
                      ss.at[g, others[i]], sr.at[g, others[i]], home[i])

    def fwd(a, zz):
        return remote(G.at[a, zz, pl.ds(0, 2)], H.at[a, zz], fs.at[a, zz], fr.at[a, zz], partner)

    def fwd_stat(g, zz):
        return remote(Gs.at[zz, group[g]], Hs.at[zz, group[g]], gs.at[g, zz], gr.at[g, zz], partner)

    def pair(p):
        return pl.ds(2 * p, 2)

    def kv_out(p, i):
        return remote(skv.at[others[i], pair(p)], okv.at[z, pair(p)],
                      ks.at[p, others[i]], kr.at[p, z], home[i])

    def kv_in(p, i):
        return remote(skv.at[others[i], pair(p)], okv.at[others[i], pair(p)],
                      ks.at[p, others[i]], kr.at[p, others[i]], home[i])

    def q_out(sl, k, i):
        return remote(sq.at[q_to[i], sl], oq.at[z, sl], qs.at[k, q_to[i]], qr.at[k, z], q_home[i])

    def q_in(sl, k, i):
        return remote(sq.at[q_to[i], sl], oq.at[q_to[i], sl], qs.at[k, q_to[i]], qr.at[k, q_to[i]], q_home[i])

    last = ((1, pl.ds(1, 1), 0), (0, pl.ds(0, 1), half))

    def cross(a):
        return remote(dqp.at[a], X.at[a], xs.at[a], xr.at[a], partner)

    def relayout(a):
        for i in range(5):
            load(a, i).wait()
        pm = perm[...]
        for b in range(2):
            rows = pl.ds(pl.multiple_of(a * 512 + b * 256, 256), 256)
            for t, ref in enumerate((q_r, do_r, k_r, v_r)):
                y = dot(pm, ref[rows, :]).astype(BF16)
                for h in range(4):
                    sb[h, a, t, b * 64:(b + 1) * 64, :] = y[h * 64:(h + 1) * 64]
            y = dot(pm, o_r[rows, :]).astype(BF16)
            for h in range(4):
                orel[h, b * 64:(b + 1) * 64, :] = y[h * 64:(h + 1) * 64]
        eye = (lax.broadcasted_iota(jnp.int32, (R, R), 0)
               == lax.broadcasted_iota(jnp.int32, (R, R), 1))
        for h in range(4):
            prod = dot(sb[h, a, 1], orel[h], NT)
            delta = jnp.sum(jnp.where(eye, prod, 0.0), axis=0, keepdims=True)
            sbs[h, a, 0:1, :] = lse_r[h:h + 1, pl.ds(pl.multiple_of(a * R, R), R)] * log2e
            sbs[h, a, 1:2, :] = delta
        G[a, z] = sb[z, a]
        Gs[z, a] = sbs[z, a]

    def send(a):
        for i in range(3):
            data(a, i).start()
        fwd(a, z).start()

    def send_stats(g):
        for i in range(3):
            stat(g, i).start()
        fwd_stat(g, z).start()

    relayout(nc - 1)
    pl.semaphore_wait(barrier, 4)
    send(nc - 1)
    send_stats(0)

    @pl.loop(1, nc)
    def _(step):
        relayout(nc - 1 - step)

    send_stats(1)

    @pl.loop(1, nc)
    def _(step):
        send(nc - 1 - step)

    iperm2[...] = interleave(256, 4)
    iperm4[...] = interleave(512, 4)

    def tile(a, b, j, diagonal):
        src, stats, dq = (G, Gs, dqo) if j < 2 else (H, Hs, dqp)
        jj = j % 2
        kk = G[a, :, 2].reshape(4 * R, D)
        vv = G[a, :, 3].reshape(4 * R, D)
        qq = src[b, 2 * jj:2 * jj + 2, 0].reshape(2 * R, D)
        dd = src[b, 2 * jj:2 * jj + 2, 1].reshape(2 * R, D)
        row = [jnp.concatenate([stats[2 * jj, b, r:r + 1, :], stats[2 * jj + 1, b, r:r + 1, :]], axis=1)
               for r in range(2)]
        s = dot(kk, qq, NT) * (scale * log2e) - row[0]
        if diagonal:
            col = lax.broadcasted_iota(jnp.int32, (1, 2 * R), 1)
            tq = (col % R) * 8 + (col // R + 2 * jj) * 2 + (c if j < 2 else 1 - c)
            rw = lax.broadcasted_iota(jnp.int32, (4 * R, 1), 0)
            tk = (rw % R) * 8 + (rw // R) * 2 + c
            s = jnp.where(tq >= tk, s, -jnp.inf)
        p = jnp.exp2(s)
        dp = dot(vv, dd, NT)
        dsb = (p * (dp - row[1])).astype(BF16)
        dv_acc[...] += dot(p.astype(BF16), dd)
        dk_acc[...] += dot(dsb, qq)
        g = dot(kt[...], dsb)
        if diagonal:
            dq[b, jj] = g
        else:
            dq[b, jj] += g

    @pl.loop(0, nc)
    def _(step):
        a = nc - 1 - step
        for i in range(3):
            data_in(a, i).wait_recv()
        for zz in others:
            fwd(a, zz).start()
        for g in range(2):
            @pl.when(step == g)
            def _():
                for i in range(3):
                    stat_in(g, i).wait_recv()
                for zz in others:
                    fwd_stat(g, zz).start()
        dk_acc[...] = jnp.zeros_like(dk_acc)
        dv_acc[...] = jnp.zeros_like(dv_acc)
        kt[...] = G[a, :, 2].reshape(4 * R, D).T

        @pl.loop(a + 1, nc)
        def _(b):
            for j in range(4):
                tile(a, b, j, False)

            @pl.when(a == 0)
            def _():
                cross(b).start()

        for zz in range(4):
            fwd(a, zz).wait_recv()
        for g in range(2):
            @pl.when(step == g)
            def _():
                for zz in range(4):
                    fwd_stat(g, zz).wait_recv()
        for j in range(4):
            tile(a, a, j, True)
        for zz in range(4):
            skv[zz, a, 0] = (dk_acc[zz * R:(zz + 1) * R, :] * scale).astype(BF16)
            skv[zz, a, 1] = dv_acc[zz * R:(zz + 1) * R, :].astype(BF16)

        @pl.when(a % 2 == 0)
        def _():
            for i in range(3):
                kv_out(a // 2, i).start()

    cross(0).start()

    def finish(b):
        cross(b).wait_recv()
        for jj in range(2):
            tot = ((dqo[b, jj] + X[b, jj]) * scale).astype(BF16)
            sq[2 * jj, b] = tot[:, :R]
            sq[2 * jj + 1, b] = tot[:, R:]

    @pl.loop(1, half)
    def _(p):
        finish(2 * p)
        finish(2 * p + 1)
        for i in range(3):
            q_out(pair(p), p, i).start()

    for b, sl, k in last:
        finish(b)
        for i in range(3):
            q_out(sl, k, i).start()

    @pl.loop(0, half)
    def _(step):
        p = half - 1 - step
        for i in range(3):
            kv_in(p, i).wait_recv()
        for e in range(2):
            a = 2 * p + e
            okv[z, a] = skv[z, a]
            for t in range(2):
                for b in range(2):
                    x = jnp.concatenate([okv[h, a, t, b * 64:(b + 1) * 64, :] for h in range(4)], axis=0)
                    rows = pl.ds(pl.multiple_of(a * 4 * R + b * 256, 256), 256)
                    (dk_o, dv_o)[t][rows, :] = dot(iperm2[...], x).astype(BF16)

    @pl.loop(0, nc)
    def _(a):
        for i in range(3):
            data(a, i).wait_send()
        for zz in range(4):
            fwd(a, zz).wait_send()
        cross(a).wait_send()

    for g in range(2):
        for i in range(3):
            stat(g, i).wait_send()
        for zz in range(4):
            fwd_stat(g, zz).wait_send()

    def merge_q(b):
        oq[z, b] = sq[z, b]
        x = jnp.concatenate([oq[h, b] for h in range(4)], axis=1)
        rows = pl.ds(pl.multiple_of(b * 4 * R, 4 * R), 4 * R)
        dq_o[rows, :] = dot(iperm4[...], x, NT).astype(BF16)

    @pl.loop(0, half)
    def _(p):
        for i in range(3):
            kv_out(p, i).wait_send()

    @pl.loop(1, half)
    def _(p):
        for i in range(3):
            q_out(pair(p), p, i).wait_send()
            q_in(pair(p), p, i).wait_recv()
        merge_q(2 * p)
        merge_q(2 * p + 1)

    for b, sl, k in last:
        for i in range(3):
            q_in(sl, k, i).wait_recv()
        merge_q(b)
    for b, sl, k in last:
        for i in range(3):
            q_out(sl, k, i).wait_send()


def place_kernel(*refs):
    src, dst, sems = refs[:3], refs[3:6], refs[6]
    n = src[0].shape[0] // 4
    copies = [pltpu.make_async_copy(src[t].at[pl.ds(i * n, n)], dst[t].at[pl.ds(i * n, n)], sems.at[t, i])
              for t in range(3) for i in range(4)]
    for x in copies:
        x.start()
    for x in copies:
        x.wait()


def solution(mesh):
    rows = P(('dp', 'cp'))
    cols = P(None, ('dp', 'cp'))

    def local(q, k, v, o, do, lse):
        n, h, d = q.shape
        nc = n // R
        flat = [x.reshape(n * h, d) for x in (q, do, k, v, o)]
        any_ = pl.BlockSpec(memory_space=pl.ANY)
        sem = pltpu.SemaphoreType.DMA
        vmem = pl.BlockSpec(memory_space=pltpu.VMEM)
        exchange = pl.pallas_call(
            functools.partial(exchange_kernel, nc),
            out_shape=(pltpu.VMEM((n * h, d), BF16),) * 3,
            in_specs=[any_] * 6,
            out_specs=(vmem,) * 3,
            scratch_shapes=[pltpu.VMEM((n * h, d), BF16)] * 5 + [
                pltpu.VMEM((4, n), F32),
                pltpu.VMEM((256, 256), BF16),
                pltpu.VMEM((256, 256), BF16),
                pltpu.VMEM((512, 512), BF16),
                pltpu.VMEM((4, R, D), BF16),
                pltpu.VMEM((4, nc, 4, R, D), BF16),
                pltpu.VMEM((4, nc, 2, R), F32),
                pltpu.VMEM((nc, 4, 4, R, D), BF16),
                pltpu.VMEM((4, nc, 2, R), F32),
                pltpu.VMEM((nc, 4, 2, R, D), BF16),
                pltpu.VMEM((4, nc, 2, R), F32),
                pltpu.VMEM((D, 4 * R), BF16),
                pltpu.VMEM((4 * R, D), F32),
                pltpu.VMEM((4 * R, D), F32),
                pltpu.VMEM((nc, 2, D, 2 * R), F32),
                pltpu.VMEM((nc, 2, D, 2 * R), F32),
                pltpu.VMEM((nc, 2, D, 2 * R), F32),
                pltpu.VMEM((4, nc, 2, R, D), BF16),
                pltpu.VMEM((4, nc, D, R), BF16),
                pltpu.VMEM((4, nc, 2, R, D), BF16),
                pltpu.VMEM((4, nc, D, R), BF16),
                sem((1,)), sem((nc, 5)),
            ] + [sem((nc, 4))] * 2 + [sem((2, 4))] * 2 + [sem((nc, 4))] * 2 + [sem((2, 4))] * 2 + [
                sem((nc // 2, 4))] * 2 + [sem((nc // 2 + 1, 4))] * 2 + [sem((nc,))] * 2,
            compiler_params=pltpu.CompilerParams(collective_id=0, has_side_effects=True,
                                                 vmem_limit_bytes=56 * 2 ** 20),
            name='exchange',
        )
        dq, dk, dv = exchange(*flat, lse)
        outs = [pltpu.with_memory_space_constraint(x, pltpu.VMEM) for x in (dq, dk, dv)]
        dq, dk, dv = pl.pallas_call(
            place_kernel,
            out_shape=(jax.ShapeDtypeStruct((n * h, d), BF16),) * 3,
            in_specs=[any_] * 3,
            out_specs=(any_,) * 3,
            scratch_shapes=[sem((3, 4))],
            name='place',
        )(*outs)
        return tuple(x.reshape(n, h, d) for x in (dq, dk, dv))

    return jax.shard_map(local, mesh=mesh,
                         in_specs=(rows, rows, rows, rows, rows, cols),
                         out_specs=(rows, rows, rows), check_vma=False)
```
